1024 devices in a mesh: gx: 8 (over x, core), gy: 128 (over y, z).
Axes of the slice: x: 4, y: 8, z: 16, core: 2. Of those that a mesh axis runs over, the one named last changes fastest.
Arguments:
- right_side: float32 [65536, 128], P(('gx', 'gy')), may hold values from -21 to 21
- mass: float32 [65536, 128], P(('gx', 'gy')), may hold values from 0.5 to 2
- edge_coeff: float32 [65536, 6, 128], P(('gx', 'gy')), may hold values from 0.05 to 0.4
- cell_edges: int32 [65536, 6], P(('gx', 'gy')), may hold values from 0 to 191, as said below
- halo_blocks: int32 [1024, 4, 32], P(('gx', 'gy')), may hold values from 0 to 63, as said below
Outputs:
- solution_field: float32 [65536, 128], P(('gx', 'gy'))
- residual_norm: float32 [], replicated
The draws below stay inside these ranges and needn't reach their ends.
Inputs may be any that keep to these rules, and one draw needn't show every extreme that they name: `halo_blocks`: for each partition and each of the four directions, 32 distinct local blocks of that partition. `cell_edges`: an entry below 64 names another local block of the same partition, never the row's own block; a larger entry names a block of a received group. No entry names a group from a partition that does not exist. Within a group only a leading run of its 32 blocks is named; its length differs between partitions and directions and is 32 for some partitions.
All inputs are finite; a program needn't handle non-finite values.
Results may differ from the reference program's by a relative error of at most 0.0001.
Values sent between devices are 32-bit elements; how exact they have to be, the bound alone decides.
No kernel may reach another device: no remote copies, remote signals or barrier semaphores. Data moves between devices by JAX's collectives and lax.ppermute only.
A program may use at most 32 MiB of HBM per device.

```python
import math
import jax
import jax.numpy as jnp
from jax import lax

BLK_DEV = 64
EDG = 6
HB = 32
ITERS = 4
NBLK = 65536
N_GX = 8
N_GY = 128


def draw_right_side(key, part):
    parts = N_GX * N_GY
    owner = (jnp.arange(parts * BLK_DEV) // BLK_DEV).astype(jnp.float32)
    rise = 1.0 + 2.0 * owner / max(parts - 1, 1)
    noise = jnp.clip(jax.random.normal(key, (parts * BLK_DEV, 128), jnp.float32), -4.0, 4.0)
    return noise * rise[:, None]


def draw_halo_blocks(key, part):
    parts = N_GX * N_GY
    scores = jax.random.randint(key, (parts, 4, BLK_DEV), 0, 1 << 20) * BLK_DEV + jnp.arange(BLK_DEV)
    order = jnp.argsort(scores, axis=-1, stable=True)
    return order[:, :, :HB].astype(jnp.int32)


def draw_cell_edges(key, part):
    parts = N_GX * N_GY
    lowest = max(HB // 4, 1)
    counts = jax.random.randint(jax.random.fold_in(key, 7), (parts, 4), lowest, HB + 1)
    counts = jnp.where((jnp.arange(parts) % 5 == 0)[:, None], HB, counts)

    def one_partition(index):
        keys = jax.random.split(jax.random.fold_in(key, index), 4)
        shape = (BLK_DEV, EDG)
        own = jnp.arange(BLK_DEV)[:, None]
        pick = jax.random.randint(keys[0], shape, 0, BLK_DEV - 1)
        pick = jnp.where(pick >= own, pick + 1, pick)
        direction = jax.random.randint(keys[1], shape, 0, 4)
        column = index % N_GY
        row_index = index // N_GY
        present = jnp.stack([column > 0, column < N_GY - 1, row_index > 0, row_index < N_GX - 1])
        limit = counts[index]
        slot = jax.random.randint(keys[2], shape, 0, 1 << 20) % limit[direction]
        remote = (jax.random.randint(keys[3], shape, 0, 4) == 0) & present[direction]
        target = BLK_DEV + direction * HB + slot
        return jnp.where(remote, target, pick).astype(jnp.int32)
    return lax.map(one_partition, jnp.arange(parts)).reshape(parts * BLK_DEV, EDG)


def steps_of(own_key, shape, pieces, low, top_value):
    factor_of = 1.0
    for position, blocks in pieces:
        draws = jax.random.uniform(jax.random.fold_in(jax.random.fold_in(own_key, 6), position), (blocks,), jnp.float32, low / len(pieces), top_value / len(pieces))
        factor_of = factor_of * jnp.repeat(jnp.exp(draws), shape[position] // blocks).reshape((-1,) + (1,) * (len(shape) - 1 - position))
    return factor_of


def setup_inputs(seed: int = 0) -> dict:
    key_of = jax.random.split(jax.random.key(seed), 6)
    return {
        "right_side": draw_right_side(jax.random.fold_in(key_of[5], 71), 0),
        "mass": jnp.clip(jnp.exp(math.log(2.0) - 1.3862944 * jax.random.uniform(key_of[1], (NBLK, 128), jnp.float32) ** steps_of(key_of[1], (NBLK, 128), ((0, 1024),), -0.2, 0.2)), 0.5, 2.0),
        "edge_coeff": jnp.clip(jnp.exp(math.log(0.4) - 2.0794415 * jax.random.uniform(key_of[2], (NBLK, EDG, 128), jnp.float32) ** steps_of(key_of[2], (NBLK, EDG, 128), ((0, 1024),), -0.2, 0.2)), 0.05, 0.4),
        "cell_edges": draw_cell_edges(jax.random.fold_in(key_of[5], 71), 0),
        "halo_blocks": draw_halo_blocks(jax.random.fold_in(key_of[5], 71), 0),
    }


spectrum_low = 0.5
spectrum_high = 7.0
lane_shifts = (1, -1, 3, -3, 5, -5)

def rotate_lanes(beside):
    rows = [jnp.roll(beside[:, e, :], -lane_shifts[e], axis=-1) for e in range(beside.shape[1])]
    return jnp.stack(rows, axis=1)

def extended_lists(field, halo_blocks):
    parts = N_GX * N_GY
    grid = field.reshape(parts, BLK_DEV, 128)
    packed = jax.vmap(lambda blocks, chosen: blocks[chosen])(grid, halo_blocks)
    packed = packed.reshape(N_GX, N_GY, 4, HB, 128)
    low_y = jnp.pad(packed[:, :-1, 0], ((0, 0), (1, 0), (0, 0), (0, 0)))
    high_y = jnp.pad(packed[:, 1:, 1], ((0, 0), (0, 1), (0, 0), (0, 0)))
    low_x = jnp.pad(packed[:-1, :, 2], ((1, 0), (0, 0), (0, 0), (0, 0)))
    high_x = jnp.pad(packed[1:, :, 3], ((0, 1), (0, 0), (0, 0), (0, 0)))
    groups = jnp.stack([low_y, high_y, low_x, high_x], axis=2).reshape(parts, 4 * HB, 128)
    return jnp.concatenate([grid, groups], axis=1)

def apply_operator(field, mass, edge_coeff, cell_edges, halo_blocks):
    parts = N_GX * N_GY
    extended = extended_lists(field, halo_blocks)

    def one_partition(items):
        values, edges, coeff, own, diag = items
        beside = rotate_lanes(values[edges])
        return diag * own + lax.optimization_barrier(jnp.sum(coeff * (own[:, None, :] - beside), axis=1))
    result = lax.map(one_partition, (extended, cell_edges.reshape(parts, BLK_DEV, EDG), edge_coeff.reshape(parts, BLK_DEV, EDG, 128), field.reshape(parts, BLK_DEV, 128), mass.reshape(parts, BLK_DEV, 128)))
    return result.reshape(parts * BLK_DEV, 128)

def reference(right_side, mass, edge_coeff, cell_edges, halo_blocks):
    theta = (spectrum_high + spectrum_low) / 2.0
    delta = (spectrum_high - spectrum_low) / 2.0
    sigma = theta / delta
    rho = 1.0 / sigma
    solution_field = jnp.zeros_like(right_side)
    residual = right_side
    direction = residual / theta
    for step in range(ITERS):
        image = apply_operator(direction, mass, edge_coeff, cell_edges, halo_blocks)
        solution_field = solution_field + direction
        residual = residual - image
        if step + 1 < ITERS:
            rho_next = 1.0 / (2.0 * sigma - rho)
            direction = rho_next * rho * direction + 2.0 * rho_next / delta * residual
            rho = rho_next
    true_residual = right_side - apply_operator(solution_field, mass, edge_coeff, cell_edges, halo_blocks)
    cells_all = right_side.shape[0] * 128
    residual_norm = jnp.sqrt(jnp.sum(true_residual * true_residual) / cells_all + 1e-06)
    return (solution_field, residual_norm)
```

```python
import jax
import jax.numpy as jnp
from jax import lax
from jax.experimental import pallas as pl
from jax.experimental.pallas import tpu as pltpu
from jax.sharding import Mesh
from jax.sharding import PartitionSpec as P

ITERS = 4
EDG = 6
BLK = 64
HB = 32
GY = ("gy_0", "gy_1")
GX = ("gx_0", "gx_1")
GX_GY = ("gx_0", "gx_1", "gy_0", "gy_1")
NEAR = ("gx_0", "gx_1", "gy_0")
FAR = ("gy_1",)

spectrum_low = 0.5
spectrum_high = 7.0
lane_shifts = (1, -1, 3, -3, 5, -5)

theta = (spectrum_high + spectrum_low) / 2.0
delta = (spectrum_high - spectrum_low) / 2.0
sigma = theta / delta
PARAMS = pltpu.CompilerParams(vmem_limit_bytes=8 * 1024 * 1024)


def f32(*shape):
    return jax.ShapeDtypeStruct(shape, jnp.float32)


def call(kernel, outs, *args):
    spec = pl.BlockSpec(memory_space=pltpu.VMEM)
    return pl.pallas_call(
        kernel,
        out_shape=outs,
        in_specs=[spec] * len(args),
        out_specs=jax.tree.map(lambda _: spec, outs),
        compiler_params=PARAMS,
    )(*args)


def three_parts(value):
    high = value.astype(jnp.bfloat16)
    rest = value - high.astype(jnp.float32)
    middle = rest.astype(jnp.bfloat16)
    low = (rest - middle.astype(jnp.float32)).astype(jnp.bfloat16)
    return jnp.concatenate([high, middle, low], axis=1)


def chosen(one_hot, parts):
    rows = jnp.dot(one_hot, parts, preferred_element_type=jnp.float32)
    return rows[:, :128] + rows[:, 128:256] + rows[:, 256:]


def one_hot_rows(numbers, depth):
    n = numbers.shape[1]
    table = lax.broadcasted_iota(jnp.int32, (depth, n), 0) == numbers
    return table.astype(jnp.float32).T.astype(jnp.bfloat16)


def send(field, pick_ref, out_refs):
    packed = chosen(pick_ref[...], three_parts(field))
    for g in range(4):
        out_refs[g][...] = packed[g * HB : (g + 1) * HB]


def first_kernel(b_ref, list_ref, s0, s1, s2, s3, pick_ref):
    for g in range(4):
        pick_ref[g * HB : (g + 1) * HB, :] = one_hot_rows(list_ref[0, g : g + 1, :], BLK)
    send(b_ref[...] * (1.0 / theta), pick_ref, (s0, s1, s2, s3))


def table_kernel(edges_ref, mass_ref, coeff_ref, hot_ref, diag_ref):
    diag = mass_ref[...]
    for e in range(EDG):
        hot_ref[e * BLK : (e + 1) * BLK, :] = one_hot_rows(edges_ref[e : e + 1, :], BLK + 4 * HB)
        diag = diag + coeff_ref[e]
    diag_ref[...] = diag


def operate(field, groups, hot_ref, coeff_ref, diag_ref):
    extended = jnp.concatenate([field] + [g[...] for g in groups], axis=0)
    beside = chosen(hot_ref[...], three_parts(extended))
    image = diag_ref[...] * field
    for e in range(EDG):
        rows = pltpu.roll(beside[e * BLK : (e + 1) * BLK], (-lane_shifts[e]) % 128, 1)
        image = image - coeff_ref[e] * rows
    return image


def steps():
    rho = 1.0 / sigma
    found = []
    for _ in range(ITERS - 1):
        rho_next = 1.0 / (2.0 * sigma - rho)
        found.append((rho_next * rho, 2.0 * rho_next / delta))
        rho = rho_next
    return found


STEPS = steps()


def kernel_1(b_ref, g0, g1, g2, g3, hot, pick, coeff, diag, r_ref, d_ref, s0, s1, s2, s3):
    field = b_ref[...] * (1.0 / theta)
    residual = b_ref[...] - operate(field, (g0, g1, g2, g3), hot, coeff, diag)
    direction = STEPS[0][0] * field + STEPS[0][1] * residual
    send(direction, pick, (s0, s1, s2, s3))
    r_ref[...] = residual
    d_ref[...] = direction


def kernel_2(r0_ref, d0_ref, g0, g1, g2, g3, hot, pick, coeff, diag, r_ref, d_ref, s0, s1, s2, s3):
    field = d0_ref[...]
    residual = r0_ref[...] - operate(field, (g0, g1, g2, g3), hot, coeff, diag)
    direction = STEPS[1][0] * field + STEPS[1][1] * residual
    send(direction, pick, (s0, s1, s2, s3))
    r_ref[...] = residual
    d_ref[...] = direction


def kernel_3(b_ref, d1_ref, r0_ref, d0_ref, g0, g1, g2, g3, hot, pick, coeff, diag, x_ref, s0, s1, s2, s3):
    field = d0_ref[...]
    residual = r0_ref[...] - operate(field, (g0, g1, g2, g3), hot, coeff, diag)
    direction = STEPS[2][0] * field + STEPS[2][1] * residual
    solved = b_ref[...] * (1.0 / theta) + d1_ref[...] + field + direction
    send(solved, pick, (s0, s1, s2, s3))
    x_ref[...] = solved


def kernel_4(b_ref, x_ref, g0, g1, g2, g3, hot, coeff, diag, sum_ref):
    remaining = b_ref[...] - operate(x_ref[...], (g0, g1, g2, g3), hot, coeff, diag)
    sums = jnp.sum(remaining * remaining, axis=0, keepdims=True)
    sum_ref[...] = jnp.broadcast_to(sums, sum_ref.shape)


def chain(block, axis, distance):
    devices = range(lax.axis_size(axis))
    return lax.ppermute(block, axis, [(i - distance, i) for i in devices if i - distance in devices])


def cycle(block, axis, distance):
    n = lax.axis_size(axis)
    return lax.ppermute(block, axis, [(i, (i + distance) % n) for i in range(n)])


def exchange(packed):
    return (
        chain(packed[0], GY, 1),
        chain(packed[1], GY, -1),
        cycle(packed[2], GX, 1),
        cycle(packed[3], GX, -1),
    )


def shards(right_side, mass, edge_coeff, cell_edges, halo_blocks):
    coeff = jnp.transpose(edge_coeff, (1, 0, 2))
    edges = cell_edges.T
    field = f32(BLK, 128)
    sends = [f32(HB, 128)] * 4
    *packed, pick = call(first_kernel, sends + [jax.ShapeDtypeStruct((4 * HB, BLK), jnp.bfloat16)], right_side, halo_blocks)
    hot, diag = call(
        table_kernel,
        [jax.ShapeDtypeStruct((EDG * BLK, BLK + 4 * HB), jnp.bfloat16), field],
        edges, mass, coeff,
    )
    tables = (hot, pick, coeff, diag)
    r1, d1, *packed = call(kernel_1, [field, field] + sends, right_side, *exchange(packed), *tables)
    r2, d2, *packed = call(kernel_2, [field, field] + sends, r1, d1, *exchange(packed), *tables)
    solved, *packed = call(kernel_3, [field] + sends, right_side, d1, r2, d2, *exchange(packed), *tables)
    near, far = lax.axis_size(NEAR), lax.axis_size(FAR)
    part = call(kernel_4, f32(near, 128), right_side, solved, *exchange(packed), hot, coeff, diag)
    part = lax.all_to_all(part, NEAR, 0, 0, tiled=True)
    part = jnp.broadcast_to(jnp.sum(part, axis=0, keepdims=True), (far, 128))
    total = jnp.sum(lax.all_to_all(part, FAR, 0, 0, tiled=True))
    cells_all = right_side.shape[0] * 128 * near * far
    return solved, jnp.sqrt(total / cells_all + 1e-06)


def solution(mesh):
    split = Mesh(mesh.devices.reshape(4, 2, 8, 16), GX_GY)
    return jax.shard_map(
        shards,
        mesh=split,
        in_specs=(
            P(GX_GY, None),
            P(GX_GY, None),
            P(GX_GY, None, None),
            P(GX_GY, None),
            P(GX_GY, None, None),
        ),
        out_specs=(P(GX_GY, None), P()),
        check_vma=False,
    )
```

```python
import jax
import jax.numpy as jnp
from jax import lax
from jax.experimental import pallas as pl
from jax.experimental.pallas import tpu as pltpu
from jax.sharding import Mesh
from jax.sharding import PartitionSpec as P

ITERS = 4
EDG = 6
BLK = 64
HB = 32
GY = ("gy_0", "gy_1")
GX = ("gx_0", "gx_1")
GX_GY = ("gx_0", "gx_1", "gy_0", "gy_1")
NEAR = ("gx_0", "gx_1", "gy_0")
FAR = ("gy_1",)

spectrum_low = 0.5
spectrum_high = 7.0
lane_shifts = (1, -1, 3, -3, 5, -5)
ORDER = (0, 1, 2, 3)

theta = (spectrum_high + spectrum_low) / 2.0
delta = (spectrum_high - spectrum_low) / 2.0
sigma = theta / delta
PARAMS = pltpu.CompilerParams(vmem_limit_bytes=8 * 1024 * 1024)


def f32(*shape):
    return jax.ShapeDtypeStruct(shape, jnp.float32)


def call(kernel, outs, *args):
    spec = pl.BlockSpec(memory_space=pltpu.VMEM)
    return pl.pallas_call(
        kernel,
        out_shape=outs,
        in_specs=[spec] * len(args),
        out_specs=jax.tree.map(lambda _: spec, outs),
        compiler_params=PARAMS,
    )(*args)


def three_parts(value):
    high = value.astype(jnp.bfloat16)
    rest = value - high.astype(jnp.float32)
    middle = rest.astype(jnp.bfloat16)
    low = (rest - middle.astype(jnp.float32)).astype(jnp.bfloat16)
    return jnp.concatenate([high, middle, low], axis=1)


def chosen(one_hot, parts):
    rows = jnp.dot(one_hot, parts, preferred_element_type=jnp.float32)
    return rows[:, :128] + rows[:, 128:256] + rows[:, 256:]


def one_hot_rows(numbers, depth):
    n = numbers.shape[1]
    table = lax.broadcasted_iota(jnp.int32, (depth, n), 0) == numbers
    return table.astype(jnp.float32).T.astype(jnp.bfloat16)


def send(field, pick_ref, out_refs):
    packed = chosen(pick_ref[...], three_parts(field))
    for out_ref, g in zip(out_refs, ORDER):
        out_ref[...] = packed[g * HB : (g + 1) * HB]


def pick_kernel(list_ref, pick_ref):
    odd = lax.axis_index("gy_1") % 2 == 1
    up, down = list_ref[0, 0:1, :], list_ref[0, 1:2, :]
    rows = (jnp.where(odd, up, down), jnp.where(odd, down, up), list_ref[0, 2:3, :], list_ref[0, 3:4, :])
    for g in range(4):
        pick_ref[g * HB : (g + 1) * HB, :] = one_hot_rows(rows[g], BLK)


def first_kernel(pick_ref, b_ref, held_ref, s0, s1, s2, s3):
    held_ref[...] = b_ref[...]
    send(b_ref[...] * (1.0 / theta), pick_ref, (s0, s1, s2, s3))


def table_kernel(edges_ref, mass_ref, coeff_ref, hot_ref, diag_ref, held_ref):
    diag = mass_ref[...]
    for e in range(EDG):
        diag = diag + coeff_ref[e]
        held_ref[e] = coeff_ref[e]
    diag_ref[...] = diag
    odd = lax.axis_index("gy_1") % 2 == 1
    edges = edges_ref[...]
    edges = jnp.where(odd & (edges >= BLK) & (edges < BLK + 2 * HB), edges ^ HB, edges)
    for e in range(EDG):
        hot_ref[e * BLK : (e + 1) * BLK, :] = one_hot_rows(edges[e : e + 1, :], BLK + 4 * HB)


def copy_kernel(x_ref, y_ref):
    y_ref[...] = x_ref[...]


def operate(field, groups, hot_ref, coeff_ref, diag_ref):
    placed = {g: ref[...] for g, ref in zip(ORDER, groups)}
    extended = jnp.concatenate([field] + [placed[g] for g in range(4)], axis=0)
    beside = chosen(hot_ref[...], three_parts(extended))
    image = diag_ref[...] * field
    for e in range(EDG):
        rows = pltpu.roll(beside[e * BLK : (e + 1) * BLK], (-lane_shifts[e]) % 128, 1)
        image = image - coeff_ref[e] * rows
    return image


def steps():
    rho = 1.0 / sigma
    found = []
    for _ in range(ITERS - 1):
        rho_next = 1.0 / (2.0 * sigma - rho)
        found.append((rho_next * rho, 2.0 * rho_next / delta))
        rho = rho_next
    return found


STEPS = steps()


def kernel_1(b_ref, g0, g1, g2, g3, hot, pick, coeff, diag, r_ref, d_ref, s0, s1, s2, s3):
    field = b_ref[...] * (1.0 / theta)
    residual = b_ref[...] - operate(field, (g0, g1, g2, g3), hot, coeff, diag)
    direction = STEPS[0][0] * field + STEPS[0][1] * residual
    send(direction, pick, (s0, s1, s2, s3))
    r_ref[...] = residual
    d_ref[...] = direction


def kernel_2(r0_ref, d0_ref, g0, g1, g2, g3, hot, pick, coeff, diag, r_ref, d_ref, s0, s1, s2, s3):
    field = d0_ref[...]
    residual = r0_ref[...] - operate(field, (g0, g1, g2, g3), hot, coeff, diag)
    direction = STEPS[1][0] * field + STEPS[1][1] * residual
    send(direction, pick, (s0, s1, s2, s3))
    r_ref[...] = residual
    d_ref[...] = direction


def kernel_3(b_ref, d1_ref, r0_ref, d0_ref, g0, g1, g2, g3, hot, pick, coeff, diag, x_ref, s0, s1, s2, s3):
    field = d0_ref[...]
    residual = r0_ref[...] - operate(field, (g0, g1, g2, g3), hot, coeff, diag)
    direction = STEPS[2][0] * field + STEPS[2][1] * residual
    solved = b_ref[...] * (1.0 / theta) + d1_ref[...] + field + direction
    send(solved, pick, (s0, s1, s2, s3))
    x_ref[...] = solved


def kernel_4(b_ref, x_ref, g0, g1, g2, g3, hot, coeff, diag, sum_ref):
    remaining = b_ref[...] - operate(x_ref[...], (g0, g1, g2, g3), hot, coeff, diag)
    sums = jnp.sum(remaining * remaining, axis=0, keepdims=True)
    sum_ref[...] = jnp.broadcast_to(sums, sum_ref.shape)


def swap(block, first):
    n = lax.axis_size(GY)
    pairs = [(i, i + 1) for i in range(first, n - 1, 2)]
    return lax.ppermute(block, GY, pairs + [(j, i) for i, j in pairs])


def cycle(block, axis, distance):
    n = lax.axis_size(axis)
    return lax.ppermute(block, axis, [(i, (i + distance) % n) for i in range(n)])


def exchange(packed):
    moves = (
        lambda block: swap(block, 1),
        lambda block: swap(block, 0),
        lambda block: cycle(block, GX, 1),
        lambda block: cycle(block, GX, -1),
    )
    return [moves[g](block) for g, block in zip(ORDER, packed)]


def shards(right_side, mass, edge_coeff, cell_edges, halo_blocks):
    field = f32(BLK, 128)
    sends = [f32(HB, 128)] * 4
    pick = call(pick_kernel, jax.ShapeDtypeStruct((4 * HB, BLK), jnp.bfloat16), halo_blocks)
    held_b, *packed = call(first_kernel, [field] + sends, pick, right_side)
    hot, diag, coeff = call(
        table_kernel,
        [jax.ShapeDtypeStruct((EDG * BLK, BLK + 4 * HB), jnp.bfloat16), field, f32(EDG, BLK, 128)],
        cell_edges.T, mass, jnp.transpose(edge_coeff, (1, 0, 2)),
    )
    tables = (hot, pick, coeff, diag)
    r1, d1, *packed = call(kernel_1, [field, field] + sends, held_b, *exchange(packed), *tables)
    r2, d2, *packed = call(kernel_2, [field, field] + sends, r1, d1, *exchange(packed), *tables)
    solved, *packed = call(kernel_3, [field] + sends, held_b, d1, r2, d2, *exchange(packed), *tables)
    near, far = lax.axis_size(NEAR), lax.axis_size(FAR)
    groups, solution_field = lax.optimization_barrier((exchange(packed), call(copy_kernel, field, solved)))
    part = call(kernel_4, f32(near, 128), held_b, solved, *groups, hot, coeff, diag)
    part = lax.all_to_all(part, NEAR, 0, 0, tiled=True)
    part = jnp.broadcast_to(jnp.sum(part, axis=0, keepdims=True), (far, 128))
    total = jnp.sum(lax.all_to_all(part, FAR, 0, 0, tiled=True))
    cells_all = right_side.shape[0] * 128 * near * far
    return solution_field, jnp.sqrt(total / cells_all + 1e-06)


def solution(mesh):
    split = Mesh(mesh.devices.reshape(4, 2, 8, 16), GX_GY)
    return jax.shard_map(
        shards,
        mesh=split,
        in_specs=(
            P(GX_GY, None),
            P(GX_GY, None),
            P(GX_GY, None, None),
            P(GX_GY, None),
            P(GX_GY, None, None),
        ),
        out_specs=(P(GX_GY, None), P()),
        check_vma=False,
    )
```

```python
import jax
import jax.numpy as jnp
from jax import lax
from jax.experimental import pallas as pl
from jax.experimental.pallas import tpu as pltpu
from jax.sharding import Mesh
from jax.sharding import PartitionSpec as P

ITERS = 4
EDG = 6
BLK = 64
HB = 32
GY = ("gy_0", "gy_1")
GX = ("gx_0", "gx_1")
GX_GY = ("gx_0", "gx_1", "gy_0", "gy_1")
NEAR = ("gx_0", "gx_1", "gy_0")
FAR = ("gy_1",)

spectrum_low = 0.5
spectrum_high = 7.0
lane_shifts = (1, -1, 3, -3, 5, -5)
ORDER = (2, 0, 1, 3)

theta = (spectrum_high + spectrum_low) / 2.0
delta = (spectrum_high - spectrum_low) / 2.0
sigma = theta / delta
PARAMS = pltpu.CompilerParams(vmem_limit_bytes=8 * 1024 * 1024)


def f32(*shape):
    return jax.ShapeDtypeStruct(shape, jnp.float32)


def call(kernel, outs, *args):
    spec = pl.BlockSpec(memory_space=pltpu.VMEM)
    return pl.pallas_call(
        kernel,
        out_shape=outs,
        in_specs=[spec] * len(args),
        out_specs=jax.tree.map(lambda _: spec, outs),
        compiler_params=PARAMS,
    )(*args)


def three_parts(value):
    high = value.astype(jnp.bfloat16)
    rest = value - high.astype(jnp.float32)
    middle = rest.astype(jnp.bfloat16)
    low = (rest - middle.astype(jnp.float32)).astype(jnp.bfloat16)
    return jnp.concatenate([high, middle, low], axis=1)


def chosen(one_hot, parts):
    rows = jnp.dot(one_hot, parts, preferred_element_type=jnp.float32)
    return rows[:, :128] + rows[:, 128:256] + rows[:, 256:]


def one_hot_rows(numbers, depth):
    n = numbers.shape[1]
    table = lax.broadcasted_iota(jnp.int32, (depth, n), 0) == numbers
    return table.astype(jnp.float32).T.astype(jnp.bfloat16)


def send(field, pick_ref, out_refs):
    packed = chosen(pick_ref[...], three_parts(field))
    for out_ref, g in zip(out_refs, ORDER):
        out_ref[...] = packed[g * HB : (g + 1) * HB]


def pick_kernel(list_ref, pick_ref):
    odd = lax.axis_index("gy_1") % 2 == 1
    up, down = list_ref[0, 0:1, :], list_ref[0, 1:2, :]
    rows = (jnp.where(odd, up, down), jnp.where(odd, down, up), list_ref[0, 2:3, :], list_ref[0, 3:4, :])
    for g in range(4):
        pick_ref[g * HB : (g + 1) * HB, :] = one_hot_rows(rows[g], BLK)


def first_kernel(pick_ref, b_ref, held_ref, s0, s1, s2, s3):
    held_ref[...] = b_ref[...]
    send(b_ref[...] * (1.0 / theta), pick_ref, (s0, s1, s2, s3))


def table_kernel(edges_ref, mass_ref, coeff_ref, hot_ref, diag_ref, held_ref):
    diag = mass_ref[...]
    for e in range(EDG):
        diag = diag + coeff_ref[e]
        held_ref[e] = coeff_ref[e]
    diag_ref[...] = diag
    odd = lax.axis_index("gy_1") % 2 == 1
    edges = edges_ref[...]
    edges = jnp.where(odd & (edges >= BLK) & (edges < BLK + 2 * HB), edges ^ HB, edges)
    for e in range(EDG):
        hot_ref[e * BLK : (e + 1) * BLK, :] = one_hot_rows(edges[e : e + 1, :], BLK + 4 * HB)


def copy_kernel(x_ref, y_ref):
    y_ref[...] = x_ref[...]


def operate(field, groups, hot_ref, coeff_ref, diag_ref):
    placed = {g: ref[...] for g, ref in zip(ORDER, groups)}
    extended = jnp.concatenate([field] + [placed[g] for g in range(4)], axis=0)
    beside = chosen(hot_ref[...], three_parts(extended))
    image = diag_ref[...] * field
    for e in range(EDG):
        rows = pltpu.roll(beside[e * BLK : (e + 1) * BLK], (-lane_shifts[e]) % 128, 1)
        image = image - coeff_ref[e] * rows
    return image


def steps():
    rho = 1.0 / sigma
    found = []
    for _ in range(ITERS - 1):
        rho_next = 1.0 / (2.0 * sigma - rho)
        found.append((rho_next * rho, 2.0 * rho_next / delta))
        rho = rho_next
    return found


STEPS = steps()


def kernel_1(b_ref, g0, g1, g2, g3, hot, pick, coeff, diag, r_ref, d_ref, s0, s1, s2, s3):
    field = b_ref[...] * (1.0 / theta)
    residual = b_ref[...] - operate(field, (g0, g1, g2, g3), hot, coeff, diag)
    direction = STEPS[0][0] * field + STEPS[0][1] * residual
    send(direction, pick, (s0, s1, s2, s3))
    r_ref[...] = residual
    d_ref[...] = direction


def kernel_2(r0_ref, d0_ref, g0, g1, g2, g3, hot, pick, coeff, diag, r_ref, d_ref, s0, s1, s2, s3):
    field = d0_ref[...]
    residual = r0_ref[...] - operate(field, (g0, g1, g2, g3), hot, coeff, diag)
    direction = STEPS[1][0] * field + STEPS[1][1] * residual
    send(direction, pick, (s0, s1, s2, s3))
    r_ref[...] = residual
    d_ref[...] = direction


def kernel_3(b_ref, d1_ref, r0_ref, d0_ref, g0, g1, g2, g3, hot, pick, coeff, diag, x_ref, s0, s1, s2, s3):
    field = d0_ref[...]
    residual = r0_ref[...] - operate(field, (g0, g1, g2, g3), hot, coeff, diag)
    direction = STEPS[2][0] * field + STEPS[2][1] * residual
    solved = b_ref[...] * (1.0 / theta) + d1_ref[...] + field + direction
    send(solved, pick, (s0, s1, s2, s3))
    x_ref[...] = solved


def kernel_4(b_ref, x_ref, g0, g1, g2, g3, hot, coeff, diag, sum_ref):
    remaining = b_ref[...] - operate(x_ref[...], (g0, g1, g2, g3), hot, coeff, diag)
    sums = jnp.sum(remaining * remaining, axis=0, keepdims=True)
    sum_ref[...] = jnp.broadcast_to(sums, sum_ref.shape)


def swap(block, first):
    n = lax.axis_size(GY)
    pairs = [(i, i + 1) for i in range(first, n - 1, 2)]
    return lax.ppermute(block, GY, pairs + [(j, i) for i, j in pairs])


def cycle(block, axis, distance):
    n = lax.axis_size(axis)
    return lax.ppermute(block, axis, [(i, (i + distance) % n) for i in range(n)])


def exchange(packed):
    moves = (
        lambda block: swap(block, 1),
        lambda block: swap(block, 0),
        lambda block: cycle(block, GX, 1),
        lambda block: cycle(block, GX, -1),
    )
    return [moves[g](block) for g, block in zip(ORDER, packed)]


def shards(right_side, mass, edge_coeff, cell_edges, halo_blocks):
    field = f32(BLK, 128)
    sends = [f32(HB, 128)] * 4
    pick = call(pick_kernel, jax.ShapeDtypeStruct((4 * HB, BLK), jnp.bfloat16), halo_blocks)
    held_b, *packed = call(first_kernel, [field] + sends, pick, right_side)
    hot, diag, coeff = call(
        table_kernel,
        [jax.ShapeDtypeStruct((EDG * BLK, BLK + 4 * HB), jnp.bfloat16), field, f32(EDG, BLK, 128)],
        cell_edges.T, mass, jnp.transpose(edge_coeff, (1, 0, 2)),
    )
    tables = (hot, pick, coeff, diag)
    r1, d1, *packed = call(kernel_1, [field, field] + sends, held_b, *exchange(packed), *tables)
    r2, d2, *packed = call(kernel_2, [field, field] + sends, r1, d1, *exchange(packed), *tables)
    solved, *packed = call(kernel_3, [field] + sends, held_b, d1, r2, d2, *exchange(packed), *tables)
    near, far = lax.axis_size(NEAR), lax.axis_size(FAR)
    groups, solution_field = lax.optimization_barrier((exchange(packed), call(copy_kernel, field, solved)))
    part = call(kernel_4, f32(near, 128), held_b, solved, *groups, hot, coeff, diag)
    part = lax.all_to_all(part, NEAR, 0, 0, tiled=True)
    part = jnp.broadcast_to(jnp.sum(part, axis=0, keepdims=True), (far, 128))
    total = jnp.sum(lax.all_to_all(part, FAR, 0, 0, tiled=True))
    cells_all = right_side.shape[0] * 128 * near * far
    return solution_field, jnp.sqrt(total / cells_all + 1e-06)


def solution(mesh):
    split = Mesh(mesh.devices.reshape(4, 2, 8, 16), GX_GY)
    return jax.shard_map(
        shards,
        mesh=split,
        in_specs=(
            P(GX_GY, None),
            P(GX_GY, None),
            P(GX_GY, None, None),
            P(GX_GY, None),
            P(GX_GY, None, None),
        ),
        out_specs=(P(GX_GY, None), P()),
        check_vma=False,
    )
```

```python
import jax
import jax.numpy as jnp
from jax import lax
from jax.experimental import pallas as pl
from jax.experimental.pallas import tpu as pltpu
from jax.sharding import Mesh
from jax.sharding import PartitionSpec as P

ITERS = 4
EDG = 6
BLK = 64
HB = 32
GY = ("gy_0", "gy_1")
GX = ("gx_0", "gx_1")
GX_GY = ("gx_0", "gx_1", "gy_0", "gy_1")
NEAR = ("gx_0", "gx_1", "gy_0")
FAR = ("gy_1",)

spectrum_low = 0.5
spectrum_high = 7.0
lane_shifts = (1, -1, 3, -3, 5, -5)
FIRST = ("up", 2, "down", 3)
ORDER = (2, 0, 1, 3)

theta = (spectrum_high + spectrum_low) / 2.0
delta = (spectrum_high - spectrum_low) / 2.0
sigma = theta / delta
PARAMS = pltpu.CompilerParams(vmem_limit_bytes=8 * 1024 * 1024)


def f32(*shape):
    return jax.ShapeDtypeStruct(shape, jnp.float32)


def call(kernel, outs, *args):
    spec = pl.BlockSpec(memory_space=pltpu.VMEM)
    return pl.pallas_call(
        kernel,
        out_shape=outs,
        in_specs=[spec] * len(args),
        out_specs=jax.tree.map(lambda _: spec, outs),
        compiler_params=PARAMS,
    )(*args)


def three_parts(value):
    high = value.astype(jnp.bfloat16)
    rest = value - high.astype(jnp.float32)
    middle = rest.astype(jnp.bfloat16)
    low = (rest - middle.astype(jnp.float32)).astype(jnp.bfloat16)
    return jnp.concatenate([high, middle, low], axis=1)


def chosen(one_hot, parts):
    rows = jnp.dot(one_hot, parts, preferred_element_type=jnp.float32)
    return rows[:, :128] + rows[:, 128:256] + rows[:, 256:]


def one_hot_rows(numbers, depth):
    n = numbers.shape[1]
    table = lax.broadcasted_iota(jnp.int32, (depth, n), 0) == numbers
    return table.astype(jnp.float32).T.astype(jnp.bfloat16)


def odd_row():
    return lax.axis_index("gy_1") % 2 == 1


def send(field, pick_ref, out_refs, order=ORDER):
    packed = chosen(pick_ref[...], three_parts(field))
    placed = {g: packed[g * HB : (g + 1) * HB] for g in range(4)}
    if order is FIRST:
        odd = odd_row()
        placed["up"] = jnp.where(odd, placed[0], placed[1])
        placed["down"] = jnp.where(odd, placed[1], placed[0])
    for out_ref, g in zip(out_refs, order):
        out_ref[...] = placed[g]


def pick_kernel(list_ref, pick_ref):
    odd = odd_row()
    up, down = list_ref[0, 0:1, :], list_ref[0, 1:2, :]
    rows = (jnp.where(odd, up, down), jnp.where(odd, down, up), list_ref[0, 2:3, :], list_ref[0, 3:4, :])
    for g in range(4):
        pick_ref[g * HB : (g + 1) * HB, :] = one_hot_rows(rows[g], BLK)


def first_kernel(pick_ref, b_ref, held_ref, s0, s1, s2, s3):
    held_ref[...] = b_ref[...]
    send(b_ref[...] * (1.0 / theta), pick_ref, (s0, s1, s2, s3), FIRST)


def table_kernel(edges_ref, mass_ref, coeff_ref, hot_ref, diag_ref, held_ref):
    diag = mass_ref[...]
    for e in range(EDG):
        diag = diag + coeff_ref[e]
        held_ref[e] = coeff_ref[e]
    diag_ref[...] = diag
    odd = odd_row()
    edges = edges_ref[...]
    edges = jnp.where(odd & (edges >= BLK) & (edges < BLK + 2 * HB), edges ^ HB, edges)
    for e in range(EDG):
        hot_ref[e * BLK : (e + 1) * BLK, :] = one_hot_rows(edges[e : e + 1, :], BLK + 4 * HB)


def copy_kernel(x_ref, y_ref):
    y_ref[...] = x_ref[...]


def operate(field, groups, hot_ref, coeff_ref, diag_ref, order=ORDER):
    placed = {g: ref[...] for g, ref in zip(order, groups)}
    if order is FIRST:
        odd = odd_row()
        placed[0] = jnp.where(odd, placed["down"], placed["up"])
        placed[1] = jnp.where(odd, placed["up"], placed["down"])
    extended = jnp.concatenate([field] + [placed[g] for g in range(4)], axis=0)
    beside = chosen(hot_ref[...], three_parts(extended))
    image = diag_ref[...] * field
    for e in range(EDG):
        rows = pltpu.roll(beside[e * BLK : (e + 1) * BLK], (-lane_shifts[e]) % 128, 1)
        image = image - coeff_ref[e] * rows
    return image


def steps():
    rho = 1.0 / sigma
    found = []
    for _ in range(ITERS - 1):
        rho_next = 1.0 / (2.0 * sigma - rho)
        found.append((rho_next * rho, 2.0 * rho_next / delta))
        rho = rho_next
    return found


STEPS = steps()


def kernel_1(b_ref, g0, g1, g2, g3, hot, pick, coeff, diag, r_ref, d_ref, s0, s1, s2, s3):
    field = b_ref[...] * (1.0 / theta)
    residual = b_ref[...] - operate(field, (g0, g1, g2, g3), hot, coeff, diag, FIRST)
    direction = STEPS[0][0] * field + STEPS[0][1] * residual
    send(direction, pick, (s0, s1, s2, s3))
    r_ref[...] = residual
    d_ref[...] = direction


def kernel_2(r0_ref, d0_ref, g0, g1, g2, g3, hot, pick, coeff, diag, r_ref, d_ref, s0, s1, s2, s3):
    field = d0_ref[...]
    residual = r0_ref[...] - operate(field, (g0, g1, g2, g3), hot, coeff, diag)
    direction = STEPS[1][0] * field + STEPS[1][1] * residual
    send(direction, pick, (s0, s1, s2, s3))
    r_ref[...] = residual
    d_ref[...] = direction


def kernel_3(b_ref, d1_ref, r0_ref, d0_ref, g0, g1, g2, g3, hot, pick, coeff, diag, x_ref, s0, s1, s2, s3):
    field = d0_ref[...]
    residual = r0_ref[...] - operate(field, (g0, g1, g2, g3), hot, coeff, diag)
    direction = STEPS[2][0] * field + STEPS[2][1] * residual
    solved = b_ref[...] * (1.0 / theta) + d1_ref[...] + field + direction
    send(solved, pick, (s0, s1, s2, s3))
    x_ref[...] = solved


def kernel_4(b_ref, x_ref, g0, g1, g2, g3, hot, coeff, diag, sum_ref):
    remaining = b_ref[...] - operate(x_ref[...], (g0, g1, g2, g3), hot, coeff, diag)
    sums = jnp.sum(remaining * remaining, axis=0, keepdims=True)
    sum_ref[...] = jnp.broadcast_to(sums, sum_ref.shape)


def swap(block, first):
    n = lax.axis_size(GY)
    pairs = [(i, i + 1) for i in range(first, n - 1, 2)]
    return lax.ppermute(block, GY, pairs + [(j, i) for i, j in pairs])


def cycle(block, axis, distance):
    n = lax.axis_size(axis)
    return lax.ppermute(block, axis, [(i, (i + distance) % n) for i in range(n)])


def chain(block, axis, distance):
    n = lax.axis_size(axis)
    return lax.ppermute(block, axis, [(i - distance, i) for i in range(n) if 0 <= i - distance < n])


def exchange(packed, order=ORDER):
    moves = {
        0: lambda block: swap(block, 1),
        1: lambda block: swap(block, 0),
        2: lambda block: cycle(block, GX, 1),
        3: lambda block: cycle(block, GX, -1),
        "up": lambda block: chain(block, GY, 1),
        "down": lambda block: chain(block, GY, -1),
    }
    return [moves[g](block) for g, block in zip(order, packed)]


def shards(right_side, mass, edge_coeff, cell_edges, halo_blocks):
    field = f32(BLK, 128)
    sends = [f32(HB, 128)] * 4
    pick = call(pick_kernel, jax.ShapeDtypeStruct((4 * HB, BLK), jnp.bfloat16), halo_blocks)
    held_b, *packed = call(first_kernel, [field] + sends, pick, right_side)
    hot, diag, coeff = call(
        table_kernel,
        [jax.ShapeDtypeStruct((EDG * BLK, BLK + 4 * HB), jnp.bfloat16), field, f32(EDG, BLK, 128)],
        cell_edges.T, mass, jnp.transpose(edge_coeff, (1, 0, 2)),
    )
    tables = (hot, pick, coeff, diag)
    r1, d1, *packed = call(kernel_1, [field, field] + sends, held_b, *exchange(packed, FIRST), *tables)
    r2, d2, *packed = call(kernel_2, [field, field] + sends, r1, d1, *exchange(packed), *tables)
    solved, *packed = call(kernel_3, [field] + sends, held_b, d1, r2, d2, *exchange(packed), *tables)
    near, far = lax.axis_size(NEAR), lax.axis_size(FAR)
    groups, solution_field = lax.optimization_barrier((exchange(packed), call(copy_kernel, field, solved)))
    part = call(kernel_4, f32(near, 128), held_b, solved, *groups, hot, coeff, diag)
    part = lax.all_to_all(part, NEAR, 0, 0, tiled=True)
    part = jnp.broadcast_to(jnp.sum(part, axis=0, keepdims=True), (far, 128))
    total = jnp.sum(lax.all_to_all(part, FAR, 0, 0, tiled=True))
    cells_all = right_side.shape[0] * 128 * near * far
    return solution_field, jnp.sqrt(total / cells_all + 1e-06)


def solution(mesh):
    split = Mesh(mesh.devices.reshape(4, 2, 8, 16), GX_GY)
    return jax.shard_map(
        shards,
        mesh=split,
        in_specs=(
            P(GX_GY, None),
            P(GX_GY, None),
            P(GX_GY, None, None),
            P(GX_GY, None),
            P(GX_GY, None, None),
        ),
        out_specs=(P(GX_GY, None), P()),
        check_vma=False,
    )
```

```python
import functools

import jax
import jax.numpy as jnp
from jax import lax
from jax.experimental import pallas as pl
from jax.experimental.pallas import tpu as pltpu
from jax.sharding import Mesh
from jax.sharding import PartitionSpec as P

ITERS = 4
EDG = 6
BLK = 64
HB = 32
GY = ("gy_0", "gy_1")
GX = ("gx_0", "gx_1")
GX_GY = ("gx_0", "gx_1", "gy_0", "gy_1")
NEAR = ("gx_0", "gx_1", "gy_0")
FAR = ("gy_1",)

spectrum_low = 0.5
spectrum_high = 7.0
lane_shifts = (1, -1, 3, -3, 5, -5)
ORDER = (2, 0, 1, 3)

theta = (spectrum_high + spectrum_low) / 2.0
delta = (spectrum_high - spectrum_low) / 2.0
sigma = theta / delta
PARAMS = pltpu.CompilerParams(vmem_limit_bytes=8 * 1024 * 1024)


def f32(*shape):
    return jax.ShapeDtypeStruct(shape, jnp.float32)


def call(kernel, outs, *args):
    spec = pl.BlockSpec(memory_space=pltpu.VMEM)
    return pl.pallas_call(
        kernel,
        out_shape=outs,
        in_specs=[spec] * len(args),
        out_specs=jax.tree.map(lambda _: spec, outs),
        compiler_params=PARAMS,
    )(*args)


def three_parts(value):
    high = value.astype(jnp.bfloat16)
    rest = value - high.astype(jnp.float32)
    middle = rest.astype(jnp.bfloat16)
    low = (rest - middle.astype(jnp.float32)).astype(jnp.bfloat16)
    return jnp.concatenate([high, middle, low], axis=1)


def chosen(one_hot, parts):
    rows = jnp.dot(one_hot, parts, preferred_element_type=jnp.float32)
    return rows[:, :128] + rows[:, 128:256] + rows[:, 256:]


def one_hot_rows(numbers, depth):
    n = numbers.shape[1]
    table = lax.broadcasted_iota(jnp.int32, (depth, n), 0) == numbers
    return table.astype(jnp.float32).T.astype(jnp.bfloat16)


def send(field, pick_ref, out_refs):
    packed = chosen(pick_ref[...], three_parts(field))
    for out_ref, g in zip(out_refs, ORDER):
        out_ref[...] = packed[g * HB : (g + 1) * HB]


def pick_kernel(list_ref, pick_ref):
    odd = lax.axis_index("gy_1") % 2 == 1
    up, down = list_ref[0, 0:1, :], list_ref[0, 1:2, :]
    rows = (jnp.where(odd, up, down), jnp.where(odd, down, up), list_ref[0, 2:3, :], list_ref[0, 3:4, :])
    for g in range(4):
        pick_ref[g * HB : (g + 1) * HB, :] = one_hot_rows(rows[g], BLK)


def first_kernel(pick_ref, b_ref, held_ref, s0, s1, s2, s3):
    held_ref[...] = b_ref[...]
    send(b_ref[...] * (1.0 / theta), pick_ref, (s0, s1, s2, s3))


def table_kernel(edges_ref, mass_ref, coeff_ref, hot_ref, diag_ref, held_ref):
    diag = mass_ref[...]
    for e in range(EDG):
        diag = diag + coeff_ref[e]
        held_ref[e] = coeff_ref[e]
    diag_ref[...] = diag
    odd = lax.axis_index("gy_1") % 2 == 1
    edges = edges_ref[...]
    edges = jnp.where(odd & (edges >= BLK) & (edges < BLK + 2 * HB), edges ^ HB, edges)
    for e in range(EDG):
        hot_ref[e * BLK : (e + 1) * BLK, :] = one_hot_rows(edges[e : e + 1, :], BLK + 4 * HB)


def copy_kernel(x_ref, y_ref):
    y_ref[...] = x_ref[...]


def operate(field, groups, hot_ref, coeff_ref, diag_ref):
    placed = {g: ref[...] for g, ref in zip(ORDER, groups)}
    extended = jnp.concatenate([field] + [placed[g] for g in range(4)], axis=0)
    beside = chosen(hot_ref[...], three_parts(extended))
    image = diag_ref[...] * field
    for e in range(EDG):
        rows = pltpu.roll(beside[e * BLK : (e + 1) * BLK], (-lane_shifts[e]) % 128, 1)
        image = image - coeff_ref[e] * rows
    return image


def steps():
    rho = 1.0 / sigma
    found = []
    for _ in range(ITERS - 1):
        rho_next = 1.0 / (2.0 * sigma - rho)
        found.append((rho_next * rho, 2.0 * rho_next / delta))
        rho = rho_next
    return found


STEPS = steps()


def kernel_1(b_ref, g0, g1, g2, g3, hot, pick, coeff, diag, r_ref, d_ref, s0, s1, s2, s3):
    field = b_ref[...] * (1.0 / theta)
    residual = b_ref[...] - operate(field, (g0, g1, g2, g3), hot, coeff, diag)
    direction = STEPS[0][0] * field + STEPS[0][1] * residual
    send(direction, pick, (s0, s1, s2, s3))
    r_ref[...] = residual
    d_ref[...] = direction


def kernel_2(r0_ref, d0_ref, g0, g1, g2, g3, hot, pick, coeff, diag, r_ref, d_ref, s0, s1, s2, s3):
    field = d0_ref[...]
    residual = r0_ref[...] - operate(field, (g0, g1, g2, g3), hot, coeff, diag)
    direction = STEPS[1][0] * field + STEPS[1][1] * residual
    send(direction, pick, (s0, s1, s2, s3))
    r_ref[...] = residual
    d_ref[...] = direction


def kernel_3(b_ref, d1_ref, r0_ref, d0_ref, g0, g1, g2, g3, hot, pick, coeff, diag, x_ref, s0, s1, s2, s3):
    field = d0_ref[...]
    residual = r0_ref[...] - operate(field, (g0, g1, g2, g3), hot, coeff, diag)
    direction = STEPS[2][0] * field + STEPS[2][1] * residual
    solved = b_ref[...] * (1.0 / theta) + d1_ref[...] + field + direction
    send(solved, pick, (s0, s1, s2, s3))
    x_ref[...] = solved


def kernel_4(b_ref, x_ref, g0, g1, g2, g3, hot, coeff, diag, sum_ref):
    remaining = b_ref[...] - operate(x_ref[...], (g0, g1, g2, g3), hot, coeff, diag)
    sums = jnp.sum(remaining * remaining, axis=0, keepdims=True)
    sum_ref[...] = jnp.broadcast_to(sums, sum_ref.shape)


def norm_kernel(cells, part_ref, norm_ref):
    mean = jnp.sum(part_ref[...], keepdims=True) / cells
    norm_ref[0, 0] = jnp.sqrt(mean + 1e-06)[0, 0]


def swap(block, first):
    n = lax.axis_size(GY)
    pairs = [(i, i + 1) for i in range(first, n - 1, 2)]
    return lax.ppermute(block, GY, pairs + [(j, i) for i, j in pairs])


def cycle(block, axis, distance):
    n = lax.axis_size(axis)
    return lax.ppermute(block, axis, [(i, (i + distance) % n) for i in range(n)])


def exchange(packed):
    moves = (
        lambda block: swap(block, 1),
        lambda block: swap(block, 0),
        lambda block: cycle(block, GX, 1),
        lambda block: cycle(block, GX, -1),
    )
    return [moves[g](block) for g, block in zip(ORDER, packed)]


def shards(right_side, mass, edge_coeff, cell_edges, halo_blocks):
    field = f32(BLK, 128)
    sends = [f32(HB, 128)] * 4
    pick = call(pick_kernel, jax.ShapeDtypeStruct((4 * HB, BLK), jnp.bfloat16), halo_blocks)
    held_b, *packed = call(first_kernel, [field] + sends, pick, right_side)
    hot, diag, coeff = call(
        table_kernel,
        [jax.ShapeDtypeStruct((EDG * BLK, BLK + 4 * HB), jnp.bfloat16), field, f32(EDG, BLK, 128)],
        cell_edges.T, mass, jnp.transpose(edge_coeff, (1, 0, 2)),
    )
    tables = (hot, pick, coeff, diag)
    r1, d1, *packed = call(kernel_1, [field, field] + sends, held_b, *exchange(packed), *tables)
    r2, d2, *packed = call(kernel_2, [field, field] + sends, r1, d1, *exchange(packed), *tables)
    solved, *packed = call(kernel_3, [field] + sends, held_b, d1, r2, d2, *exchange(packed), *tables)
    near, far = lax.axis_size(NEAR), lax.axis_size(FAR)
    groups, solution_field = lax.optimization_barrier((exchange(packed), call(copy_kernel, field, solved)))
    part = call(kernel_4, f32(near, 128), held_b, solved, *groups, hot, coeff, diag)
    part = lax.all_to_all(part, NEAR, 0, 0, tiled=True)
    part = jnp.broadcast_to(jnp.sum(part, axis=0, keepdims=True), (far, 128))
    part = lax.all_to_all(part, FAR, 0, 0, tiled=True)
    cells_all = right_side.shape[0] * 128 * near * far
    norm = pl.pallas_call(
        functools.partial(norm_kernel, float(cells_all)),
        out_shape=f32(1, 1),
        in_specs=[pl.BlockSpec(memory_space=pltpu.VMEM)],
        out_specs=pl.BlockSpec(memory_space=pltpu.SMEM),
        compiler_params=PARAMS,
    )(part)
    return solution_field, norm.reshape(())


def solution(mesh):
    split = Mesh(mesh.devices.reshape(4, 2, 8, 16), GX_GY)
    return jax.shard_map(
        shards,
        mesh=split,
        in_specs=(
            P(GX_GY, None),
            P(GX_GY, None),
            P(GX_GY, None, None),
            P(GX_GY, None),
            P(GX_GY, None, None),
        ),
        out_specs=(P(GX_GY, None), P()),
        check_vma=False,
    )
```

```python
import functools

import jax
import jax.numpy as jnp
from jax import lax
from jax.experimental import pallas as pl
from jax.experimental.pallas import tpu as pltpu
from jax.sharding import Mesh
from jax.sharding import PartitionSpec as P

ITERS = 4
EDG = 6
BLK = 64
HB = 32
GY = ("gy_0", "gy_1")
GX = ("gx_0", "gx_1")
GX_GY = ("gx_0", "gx_1", "gy_0", "gy_1")
NEAR = ("gx_0", "gy_0")
FAR = ("gx_1", "gy_1")

spectrum_low = 0.5
spectrum_high = 7.0
lane_shifts = (1, -1, 3, -3, 5, -5)
ORDER = (2, 0, 1, 3)

theta = (spectrum_high + spectrum_low) / 2.0
delta = (spectrum_high - spectrum_low) / 2.0
sigma = theta / delta
PARAMS = pltpu.CompilerParams(vmem_limit_bytes=8 * 1024 * 1024)


def f32(*shape):
    return jax.ShapeDtypeStruct(shape, jnp.float32)


def call(kernel, outs, *args):
    spec = pl.BlockSpec(memory_space=pltpu.VMEM)
    return pl.pallas_call(
        kernel,
        out_shape=outs,
        in_specs=[spec] * len(args),
        out_specs=jax.tree.map(lambda _: spec, outs),
        compiler_params=PARAMS,
    )(*args)


def three_parts(value):
    high = value.astype(jnp.bfloat16)
    rest = value - high.astype(jnp.float32)
    middle = rest.astype(jnp.bfloat16)
    low = (rest - middle.astype(jnp.float32)).astype(jnp.bfloat16)
    return jnp.concatenate([high, middle, low], axis=1)


def chosen(one_hot, parts):
    rows = jnp.dot(one_hot, parts, preferred_element_type=jnp.float32)
    return rows[:, :128] + rows[:, 128:256] + rows[:, 256:]


def one_hot_rows(numbers, depth):
    n = numbers.shape[1]
    table = lax.broadcasted_iota(jnp.int32, (depth, n), 0) == numbers
    return table.astype(jnp.float32).T.astype(jnp.bfloat16)


def send(field, pick_ref, out_refs):
    packed = chosen(pick_ref[...], three_parts(field))
    for out_ref, g in zip(out_refs, ORDER):
        out_ref[...] = packed[g * HB : (g + 1) * HB]


def pick_kernel(list_ref, pick_ref):
    odd = lax.axis_index("gy_1") % 2 == 1
    up, down = list_ref[0, 0:1, :], list_ref[0, 1:2, :]
    rows = (jnp.where(odd, up, down), jnp.where(odd, down, up), list_ref[0, 2:3, :], list_ref[0, 3:4, :])
    for g in range(4):
        pick_ref[g * HB : (g + 1) * HB, :] = one_hot_rows(rows[g], BLK)


def first_kernel(pick_ref, b_ref, held_ref, s0, s1, s2, s3):
    held_ref[...] = b_ref[...]
    send(b_ref[...] * (1.0 / theta), pick_ref, (s0, s1, s2, s3))


def table_kernel(edges_ref, mass_ref, coeff_ref, hot_ref, diag_ref, held_ref):
    diag = mass_ref[...]
    for e in range(EDG):
        diag = diag + coeff_ref[e]
        held_ref[e] = coeff_ref[e]
    diag_ref[...] = diag
    odd = lax.axis_index("gy_1") % 2 == 1
    edges = edges_ref[...]
    edges = jnp.where(odd & (edges >= BLK) & (edges < BLK + 2 * HB), edges ^ HB, edges)
    for e in range(EDG):
        hot_ref[e * BLK : (e + 1) * BLK, :] = one_hot_rows(edges[e : e + 1, :], BLK + 4 * HB)


def copy_kernel(x_ref, y_ref):
    y_ref[...] = x_ref[...]


def operate(field, groups, hot_ref, coeff_ref, diag_ref):
    placed = {g: ref[...] for g, ref in zip(ORDER, groups)}
    extended = jnp.concatenate([field] + [placed[g] for g in range(4)], axis=0)
    beside = chosen(hot_ref[...], three_parts(extended))
    image = diag_ref[...] * field
    for e in range(EDG):
        rows = pltpu.roll(beside[e * BLK : (e + 1) * BLK], (-lane_shifts[e]) % 128, 1)
        image = image - coeff_ref[e] * rows
    return image


def steps():
    rho = 1.0 / sigma
    found = []
    for _ in range(ITERS - 1):
        rho_next = 1.0 / (2.0 * sigma - rho)
        found.append((rho_next * rho, 2.0 * rho_next / delta))
        rho = rho_next
    return found


STEPS = steps()


def kernel_1(b_ref, g0, g1, g2, g3, hot, pick, coeff, diag, r_ref, d_ref, s0, s1, s2, s3):
    field = b_ref[...] * (1.0 / theta)
    residual = b_ref[...] - operate(field, (g0, g1, g2, g3), hot, coeff, diag)
    direction = STEPS[0][0] * field + STEPS[0][1] * residual
    send(direction, pick, (s0, s1, s2, s3))
    r_ref[...] = residual
    d_ref[...] = direction


def kernel_2(r0_ref, d0_ref, g0, g1, g2, g3, hot, pick, coeff, diag, r_ref, d_ref, s0, s1, s2, s3):
    field = d0_ref[...]
    residual = r0_ref[...] - operate(field, (g0, g1, g2, g3), hot, coeff, diag)
    direction = STEPS[1][0] * field + STEPS[1][1] * residual
    send(direction, pick, (s0, s1, s2, s3))
    r_ref[...] = residual
    d_ref[...] = direction


def kernel_3(b_ref, d1_ref, r0_ref, d0_ref, g0, g1, g2, g3, hot, pick, coeff, diag, x_ref, s0, s1, s2, s3):
    field = d0_ref[...]
    residual = r0_ref[...] - operate(field, (g0, g1, g2, g3), hot, coeff, diag)
    direction = STEPS[2][0] * field + STEPS[2][1] * residual
    solved = b_ref[...] * (1.0 / theta) + d1_ref[...] + field + direction
    send(solved, pick, (s0, s1, s2, s3))
    x_ref[...] = solved


def kernel_4(b_ref, x_ref, g0, g1, g2, g3, hot, coeff, diag, sum_ref):
    remaining = b_ref[...] - operate(x_ref[...], (g0, g1, g2, g3), hot, coeff, diag)
    sums = jnp.sum(remaining * remaining, axis=0, keepdims=True)
    sum_ref[...] = jnp.broadcast_to(sums, sum_ref.shape)


def norm_kernel(cells, part_ref, norm_ref):
    mean = jnp.sum(part_ref[...], keepdims=True) / cells
    norm_ref[0, 0] = jnp.sqrt(mean + 1e-06)[0, 0]


def swap(block, first):
    n = lax.axis_size(GY)
    pairs = [(i, i + 1) for i in range(first, n - 1, 2)]
    return lax.ppermute(block, GY, pairs + [(j, i) for i, j in pairs])


def cycle(block, axis, distance):
    n = lax.axis_size(axis)
    return lax.ppermute(block, axis, [(i, (i + distance) % n) for i in range(n)])


def exchange(packed):
    moves = (
        lambda block: swap(block, 1),
        lambda block: swap(block, 0),
        lambda block: cycle(block, GX, 1),
        lambda block: cycle(block, GX, -1),
    )
    return [moves[g](block) for g, block in zip(ORDER, packed)]


def shards(right_side, mass, edge_coeff, cell_edges, halo_blocks):
    field = f32(BLK, 128)
    sends = [f32(HB, 128)] * 4
    pick = call(pick_kernel, jax.ShapeDtypeStruct((4 * HB, BLK), jnp.bfloat16), halo_blocks)
    held_b, *packed = call(first_kernel, [field] + sends, pick, right_side)
    hot, diag, coeff = call(
        table_kernel,
        [jax.ShapeDtypeStruct((EDG * BLK, BLK + 4 * HB), jnp.bfloat16), field, f32(EDG, BLK, 128)],
        cell_edges.T, mass, jnp.transpose(edge_coeff, (1, 0, 2)),
    )
    tables = (hot, pick, coeff, diag)
    r1, d1, *packed = call(kernel_1, [field, field] + sends, held_b, *exchange(packed), *tables)
    r2, d2, *packed = call(kernel_2, [field, field] + sends, r1, d1, *exchange(packed), *tables)
    solved, *packed = call(kernel_3, [field] + sends, held_b, d1, r2, d2, *exchange(packed), *tables)
    near, far = lax.axis_size(NEAR), lax.axis_size(FAR)
    groups, solution_field = lax.optimization_barrier((exchange(packed), call(copy_kernel, field, solved)))
    part = call(kernel_4, f32(near, 128), held_b, solved, *groups, hot, coeff, diag)
    part = lax.all_to_all(part, NEAR, 0, 0, tiled=True)
    part = jnp.broadcast_to(jnp.sum(part, axis=0, keepdims=True), (far, 128))
    part = lax.all_to_all(part, FAR, 0, 0, tiled=True)
    cells_all = right_side.shape[0] * 128 * near * far
    norm = pl.pallas_call(
        functools.partial(norm_kernel, float(cells_all)),
        out_shape=f32(1, 1),
        in_specs=[pl.BlockSpec(memory_space=pltpu.VMEM)],
        out_specs=pl.BlockSpec(memory_space=pltpu.SMEM),
        compiler_params=PARAMS,
    )(part)
    return solution_field, norm.reshape(())


def solution(mesh):
    split = Mesh(mesh.devices.reshape(4, 2, 8, 16), GX_GY)
    return jax.shard_map(
        shards,
        mesh=split,
        in_specs=(
            P(GX_GY, None),
            P(GX_GY, None),
            P(GX_GY, None, None),
            P(GX_GY, None),
            P(GX_GY, None, None),
        ),
        out_specs=(P(GX_GY, None), P()),
        check_vma=False,
    )
```

```python
import functools

import jax
import jax.numpy as jnp
from jax import lax
from jax.experimental import pallas as pl
from jax.experimental.pallas import tpu as pltpu
from jax.sharding import Mesh
from jax.sharding import PartitionSpec as P

ITERS = 4
EDG = 6
BLK = 64
HB = 32
GY = ("gy_0", "gy_1")
GX = ("gx_0", "gx_1")
GX_GY = ("gx_0", "gx_1", "gy_0", "gy_1")
NEAR = ("gx_0", "gy_0")
FAR = ("gx_1", "gy_1")

spectrum_low = 0.5
spectrum_high = 7.0
lane_shifts = (1, -1, 3, -3, 5, -5)
ORDER = (2, 0, 1, 3)

theta = (spectrum_high + spectrum_low) / 2.0
delta = (spectrum_high - spectrum_low) / 2.0
sigma = theta / delta
PARAMS = pltpu.CompilerParams(vmem_limit_bytes=8 * 1024 * 1024)


def f32(*shape):
    return jax.ShapeDtypeStruct(shape, jnp.float32)


def call(kernel, outs, *args):
    spec = pl.BlockSpec(memory_space=pltpu.VMEM)
    return pl.pallas_call(
        kernel,
        out_shape=outs,
        in_specs=[spec] * len(args),
        out_specs=jax.tree.map(lambda _: spec, outs),
        compiler_params=PARAMS,
    )(*args)


def three_parts(value):
    high = value.astype(jnp.bfloat16)
    rest = value - high.astype(jnp.float32)
    middle = rest.astype(jnp.bfloat16)
    return jnp.concatenate([high, middle], axis=1)


def chosen(one_hot, parts):
    rows = jnp.dot(one_hot, parts, preferred_element_type=jnp.float32)
    return rows[:, :128] + rows[:, 128:]


def one_hot_rows(numbers, depth):
    n = numbers.shape[1]
    table = lax.broadcasted_iota(jnp.int32, (depth, n), 0) == numbers
    return table.astype(jnp.float32).T.astype(jnp.bfloat16)


def send(field, pick_ref, out_refs):
    packed = chosen(pick_ref[...], three_parts(field))
    for out_ref, g in zip(out_refs, ORDER):
        out_ref[...] = packed[g * HB : (g + 1) * HB]


def pick_kernel(list_ref, pick_ref):
    odd = lax.axis_index("gy_1") % 2 == 1
    up, down = list_ref[0, 0:1, :], list_ref[0, 1:2, :]
    rows = (jnp.where(odd, up, down), jnp.where(odd, down, up), list_ref[0, 2:3, :], list_ref[0, 3:4, :])
    for g in range(4):
        pick_ref[g * HB : (g + 1) * HB, :] = one_hot_rows(rows[g], BLK)


def first_kernel(pick_ref, b_ref, held_ref, s0, s1, s2, s3):
    held_ref[...] = b_ref[...]
    send(b_ref[...] * (1.0 / theta), pick_ref, (s0, s1, s2, s3))


def table_kernel(edges_ref, mass_ref, coeff_ref, hot_ref, diag_ref, held_ref):
    diag = mass_ref[...]
    for e in range(EDG):
        diag = diag + coeff_ref[e]
        held_ref[e] = coeff_ref[e]
    diag_ref[...] = diag
    odd = lax.axis_index("gy_1") % 2 == 1
    edges = edges_ref[...]
    edges = jnp.where(odd & (edges >= BLK) & (edges < BLK + 2 * HB), edges ^ HB, edges)
    for e in range(EDG):
        hot_ref[e * BLK : (e + 1) * BLK, :] = one_hot_rows(edges[e : e + 1, :], BLK + 4 * HB)


def copy_kernel(x_ref, y_ref):
    y_ref[...] = x_ref[...]


def operate(field, groups, hot_ref, coeff_ref, diag_ref):
    placed = {g: ref[...] for g, ref in zip(ORDER, groups)}
    extended = jnp.concatenate([field] + [placed[g] for g in range(4)], axis=0)
    beside = chosen(hot_ref[...], three_parts(extended))
    image = diag_ref[...] * field
    for e in range(EDG):
        rows = pltpu.roll(beside[e * BLK : (e + 1) * BLK], (-lane_shifts[e]) % 128, 1)
        image = image - coeff_ref[e] * rows
    return image


def steps():
    rho = 1.0 / sigma
    found = []
    for _ in range(ITERS - 1):
        rho_next = 1.0 / (2.0 * sigma - rho)
        found.append((rho_next * rho, 2.0 * rho_next / delta))
        rho = rho_next
    return found


STEPS = steps()


def kernel_1(b_ref, g0, g1, g2, g3, hot, pick, coeff, diag, r_ref, d_ref, s0, s1, s2, s3):
    field = b_ref[...] * (1.0 / theta)
    residual = b_ref[...] - operate(field, (g0, g1, g2, g3), hot, coeff, diag)
    direction = STEPS[0][0] * field + STEPS[0][1] * residual
    send(direction, pick, (s0, s1, s2, s3))
    r_ref[...] = residual
    d_ref[...] = direction


def kernel_2(r0_ref, d0_ref, g0, g1, g2, g3, hot, pick, coeff, diag, r_ref, d_ref, s0, s1, s2, s3):
    field = d0_ref[...]
    residual = r0_ref[...] - operate(field, (g0, g1, g2, g3), hot, coeff, diag)
    direction = STEPS[1][0] * field + STEPS[1][1] * residual
    send(direction, pick, (s0, s1, s2, s3))
    r_ref[...] = residual
    d_ref[...] = direction


def kernel_3(b_ref, d1_ref, r0_ref, d0_ref, g0, g1, g2, g3, hot, pick, coeff, diag, x_ref, s0, s1, s2, s3):
    field = d0_ref[...]
    residual = r0_ref[...] - operate(field, (g0, g1, g2, g3), hot, coeff, diag)
    direction = STEPS[2][0] * field + STEPS[2][1] * residual
    solved = b_ref[...] * (1.0 / theta) + d1_ref[...] + field + direction
    send(solved, pick, (s0, s1, s2, s3))
    x_ref[...] = solved


def kernel_4(b_ref, x_ref, g0, g1, g2, g3, hot, coeff, diag, sum_ref):
    remaining = b_ref[...] - operate(x_ref[...], (g0, g1, g2, g3), hot, coeff, diag)
    sums = jnp.sum(remaining * remaining, axis=0, keepdims=True)
    sum_ref[...] = jnp.broadcast_to(sums, sum_ref.shape)


def norm_kernel(cells, part_ref, norm_ref):
    mean = jnp.sum(part_ref[...], keepdims=True) / cells
    norm_ref[0, 0] = jnp.sqrt(mean + 1e-06)[0, 0]


def swap(block, first):
    n = lax.axis_size(GY)
    pairs = [(i, i + 1) for i in range(first, n - 1, 2)]
    return lax.ppermute(block, GY, pairs + [(j, i) for i, j in pairs])


def cycle(block, axis, distance):
    n = lax.axis_size(axis)
    return lax.ppermute(block, axis, [(i, (i + distance) % n) for i in range(n)])


def exchange(packed):
    moves = (
        lambda block: swap(block, 1),
        lambda block: swap(block, 0),
        lambda block: cycle(block, GX, 1),
        lambda block: cycle(block, GX, -1),
    )
    return [moves[g](block) for g, block in zip(ORDER, packed)]


def shards(right_side, mass, edge_coeff, cell_edges, halo_blocks):
    field = f32(BLK, 128)
    sends = [f32(HB, 128)] * 4
    pick = call(pick_kernel, jax.ShapeDtypeStruct((4 * HB, BLK), jnp.bfloat16), halo_blocks)
    held_b, *packed = call(first_kernel, [field] + sends, pick, right_side)
    hot, diag, coeff = call(
        table_kernel,
        [jax.ShapeDtypeStruct((EDG * BLK, BLK + 4 * HB), jnp.bfloat16), field, f32(EDG, BLK, 128)],
        cell_edges.T, mass, jnp.transpose(edge_coeff, (1, 0, 2)),
    )
    tables = (hot, pick, coeff, diag)
    r1, d1, *packed = call(kernel_1, [field, field] + sends, held_b, *exchange(packed), *tables)
    r2, d2, *packed = call(kernel_2, [field, field] + sends, r1, d1, *exchange(packed), *tables)
    solved, *packed = call(kernel_3, [field] + sends, held_b, d1, r2, d2, *exchange(packed), *tables)
    near, far = lax.axis_size(NEAR), lax.axis_size(FAR)
    groups, solution_field = lax.optimization_barrier((exchange(packed), call(copy_kernel, field, solved)))
    part = call(kernel_4, f32(near, 128), held_b, solved, *groups, hot, coeff, diag)
    part = lax.all_to_all(part, NEAR, 0, 0, tiled=True)
    part = jnp.broadcast_to(jnp.sum(part, axis=0, keepdims=True), (far, 128))
    part = lax.all_to_all(part, FAR, 0, 0, tiled=True)
    cells_all = right_side.shape[0] * 128 * near * far
    norm = pl.pallas_call(
        functools.partial(norm_kernel, float(cells_all)),
        out_shape=f32(1, 1),
        in_specs=[pl.BlockSpec(memory_space=pltpu.VMEM)],
        out_specs=pl.BlockSpec(memory_space=pltpu.SMEM),
        compiler_params=PARAMS,
    )(part)
    return solution_field, norm.reshape(())


def solution(mesh):
    split = Mesh(mesh.devices.reshape(4, 2, 8, 16), GX_GY)
    return jax.shard_map(
        shards,
        mesh=split,
        in_specs=(
            P(GX_GY, None),
            P(GX_GY, None),
            P(GX_GY, None, None),
            P(GX_GY, None),
            P(GX_GY, None, None),
        ),
        out_specs=(P(GX_GY, None), P()),
        check_vma=False,
    )
```

```python
import functools

import jax
import jax.numpy as jnp
from jax import lax
from jax.experimental import pallas as pl
from jax.experimental.pallas import tpu as pltpu
from jax.sharding import Mesh
from jax.sharding import PartitionSpec as P

ITERS = 4
EDG = 6
BLK = 64
HB = 32
GY = ("gy_0", "gy_1")
GX = ("gx_0", "gx_1")
GX_GY = ("gx_0", "gx_1", "gy_0", "gy_1")
NEAR = ("gx_0", "gx_1", "gy_0")
FAR = ("gy_1",)

spectrum_low = 0.5
spectrum_high = 7.0
lane_shifts = (1, -1, 3, -3, 5, -5)
ORDER = (2, 0, 1, 3)

theta = (spectrum_high + spectrum_low) / 2.0
delta = (spectrum_high - spectrum_low) / 2.0
sigma = theta / delta
PARAMS = pltpu.CompilerParams(vmem_limit_bytes=8 * 1024 * 1024)


def f32(*shape):
    return jax.ShapeDtypeStruct(shape, jnp.float32)


def call(kernel, outs, *args):
    spec = pl.BlockSpec(memory_space=pltpu.VMEM)
    return pl.pallas_call(
        kernel,
        out_shape=outs,
        in_specs=[spec] * len(args),
        out_specs=jax.tree.map(lambda _: spec, outs),
        compiler_params=PARAMS,
    )(*args)


def three_parts(value):
    high = value.astype(jnp.bfloat16)
    rest = value - high.astype(jnp.float32)
    middle = rest.astype(jnp.bfloat16)
    low = (rest - middle.astype(jnp.float32)).astype(jnp.bfloat16)
    return jnp.concatenate([high, middle, low], axis=1)


def chosen(one_hot, parts):
    rows = jnp.dot(one_hot, parts, preferred_element_type=jnp.float32)
    return rows[:, :128] + rows[:, 128:256] + rows[:, 256:]


def one_hot_rows(numbers, depth):
    n = numbers.shape[1]
    table = lax.broadcasted_iota(jnp.int32, (depth, n), 0) == numbers
    return table.astype(jnp.float32).T.astype(jnp.bfloat16)


def send(field, pick_ref, out_refs):
    packed = chosen(pick_ref[...], three_parts(field))
    for out_ref, g in zip(out_refs, ORDER):
        out_ref[...] = packed[g * HB : (g + 1) * HB]


def pick_kernel(list_ref, pick_ref):
    odd = (lax.axis_index("gy_1") + lax.axis_index("gx_1")) % 2 == 1
    up, down = list_ref[0, 0:1, :], list_ref[0, 1:2, :]
    rows = (jnp.where(odd, up, down), jnp.where(odd, down, up), list_ref[0, 2:3, :], list_ref[0, 3:4, :])
    for g in range(4):
        pick_ref[g * HB : (g + 1) * HB, :] = one_hot_rows(rows[g], BLK)


def first_kernel(pick_ref, b_ref, held_ref, s0, s1, s2, s3):
    held_ref[...] = b_ref[...]
    send(b_ref[...] * (1.0 / theta), pick_ref, (s0, s1, s2, s3))


def table_kernel(edges_ref, mass_ref, coeff_ref, hot_ref, diag_ref, held_ref):
    diag = mass_ref[...]
    for e in range(EDG):
        diag = diag + coeff_ref[e]
        held_ref[e] = coeff_ref[e]
    diag_ref[...] = diag
    odd = (lax.axis_index("gy_1") + lax.axis_index("gx_1")) % 2 == 1
    edges = edges_ref[...]
    edges = jnp.where(odd & (edges >= BLK) & (edges < BLK + 2 * HB), edges ^ HB, edges)
    for e in range(EDG):
        hot_ref[e * BLK : (e + 1) * BLK, :] = one_hot_rows(edges[e : e + 1, :], BLK + 4 * HB)


def copy_kernel(x_ref, y_ref):
    y_ref[...] = x_ref[...]


def operate(field, groups, hot_ref, coeff_ref, diag_ref):
    placed = {g: ref[...] for g, ref in zip(ORDER, groups)}
    extended = jnp.concatenate([field] + [placed[g] for g in range(4)], axis=0)
    beside = chosen(hot_ref[...], three_parts(extended))
    image = diag_ref[...] * field
    for e in range(EDG):
        rows = pltpu.roll(beside[e * BLK : (e + 1) * BLK], (-lane_shifts[e]) % 128, 1)
        image = image - coeff_ref[e] * rows
    return image


def steps():
    rho = 1.0 / sigma
    found = []
    for _ in range(ITERS - 1):
        rho_next = 1.0 / (2.0 * sigma - rho)
        found.append((rho_next * rho, 2.0 * rho_next / delta))
        rho = rho_next
    return found


STEPS = steps()


def kernel_1(b_ref, g0, g1, g2, g3, hot, pick, coeff, diag, r_ref, d_ref, s0, s1, s2, s3):
    field = b_ref[...] * (1.0 / theta)
    residual = b_ref[...] - operate(field, (g0, g1, g2, g3), hot, coeff, diag)
    direction = STEPS[0][0] * field + STEPS[0][1] * residual
    send(direction, pick, (s0, s1, s2, s3))
    r_ref[...] = residual
    d_ref[...] = direction


def kernel_2(r0_ref, d0_ref, g0, g1, g2, g3, hot, pick, coeff, diag, r_ref, d_ref, s0, s1, s2, s3):
    field = d0_ref[...]
    residual = r0_ref[...] - operate(field, (g0, g1, g2, g3), hot, coeff, diag)
    direction = STEPS[1][0] * field + STEPS[1][1] * residual
    send(direction, pick, (s0, s1, s2, s3))
    r_ref[...] = residual
    d_ref[...] = direction


def kernel_3(b_ref, d1_ref, r0_ref, d0_ref, g0, g1, g2, g3, hot, pick, coeff, diag, x_ref, s0, s1, s2, s3):
    field = d0_ref[...]
    residual = r0_ref[...] - operate(field, (g0, g1, g2, g3), hot, coeff, diag)
    direction = STEPS[2][0] * field + STEPS[2][1] * residual
    solved = b_ref[...] * (1.0 / theta) + d1_ref[...] + field + direction
    send(solved, pick, (s0, s1, s2, s3))
    x_ref[...] = solved


def kernel_4(b_ref, x_ref, g0, g1, g2, g3, hot, coeff, diag, sum_ref):
    remaining = b_ref[...] - operate(x_ref[...], (g0, g1, g2, g3), hot, coeff, diag)
    sums = jnp.sum(remaining * remaining, axis=0, keepdims=True)
    sum_ref[...] = jnp.broadcast_to(sums, sum_ref.shape)


def norm_kernel(cells, part_ref, norm_ref):
    mean = jnp.sum(part_ref[...], keepdims=True) / cells
    norm_ref[0, 0] = jnp.sqrt(mean + 1e-06)[0, 0]


def swap(block, first):
    n = lax.axis_size(GY)
    pairs = [(c * n + i, c * n + i + 1) for c in range(2) for i in range((first + c) % 2, n - 1, 2)]
    return lax.ppermute(block, ("gx_1",) + GY, pairs + [(j, i) for i, j in pairs])


def cycle(block, axis, distance):
    n = lax.axis_size(axis)
    return lax.ppermute(block, axis, [(i, (i + distance) % n) for i in range(n)])


def exchange(packed):
    moves = (
        lambda block: swap(block, 1),
        lambda block: swap(block, 0),
        lambda block: cycle(block, GX, 1),
        lambda block: cycle(block, GX, -1),
    )
    return [moves[g](block) for g, block in zip(ORDER, packed)]


def shards(right_side, mass, edge_coeff, cell_edges, halo_blocks):
    field = f32(BLK, 128)
    sends = [f32(HB, 128)] * 4
    pick = call(pick_kernel, jax.ShapeDtypeStruct((4 * HB, BLK), jnp.bfloat16), halo_blocks)
    held_b, *packed = call(first_kernel, [field] + sends, pick, right_side)
    hot, diag, coeff = call(
        table_kernel,
        [jax.ShapeDtypeStruct((EDG * BLK, BLK + 4 * HB), jnp.bfloat16), field, f32(EDG, BLK, 128)],
        cell_edges.T, mass, jnp.transpose(edge_coeff, (1, 0, 2)),
    )
    tables = (hot, pick, coeff, diag)
    r1, d1, *packed = call(kernel_1, [field, field] + sends, held_b, *exchange(packed), *tables)
    r2, d2, *packed = call(kernel_2, [field, field] + sends, r1, d1, *exchange(packed), *tables)
    solved, *packed = call(kernel_3, [field] + sends, held_b, d1, r2, d2, *exchange(packed), *tables)
    near, far = lax.axis_size(NEAR), lax.axis_size(FAR)
    groups, solution_field = lax.optimization_barrier((exchange(packed), call(copy_kernel, field, solved)))
    part = call(kernel_4, f32(near, 128), held_b, solved, *groups, hot, coeff, diag)
    part = lax.all_to_all(part, NEAR, 0, 0, tiled=True)
    part = jnp.broadcast_to(jnp.sum(part, axis=0, keepdims=True), (far, 128))
    part = lax.all_to_all(part, FAR, 0, 0, tiled=True)
    cells_all = right_side.shape[0] * 128 * near * far
    norm = pl.pallas_call(
        functools.partial(norm_kernel, float(cells_all)),
        out_shape=f32(1, 1),
        in_specs=[pl.BlockSpec(memory_space=pltpu.VMEM)],
        out_specs=pl.BlockSpec(memory_space=pltpu.SMEM),
        compiler_params=PARAMS,
    )(part)
    return solution_field, norm.reshape(())


def solution(mesh):
    split = Mesh(mesh.devices.reshape(4, 2, 8, 16), GX_GY)
    return jax.shard_map(
        shards,
        mesh=split,
        in_specs=(
            P(GX_GY, None),
            P(GX_GY, None),
            P(GX_GY, None, None),
            P(GX_GY, None),
            P(GX_GY, None, None),
        ),
        out_specs=(P(GX_GY, None), P()),
        check_vma=False,
    )
```
